128 devices in a mesh: replica: 1, data2: 16 (over z, y), data: 8 (over x, core).
Axes of the slice: x: 4, y: 4, z: 4, core: 2. Of those that a mesh axis runs over, the one named last changes fastest.
Arguments:
- query_hidden: bfloat16 [512, 32, 768], P(('replica', 'data2', 'data'))
- doc_hidden: bfloat16 [512, 512, 768], P(('replica', 'data2', 'data'))
- w_proj: bfloat16 [768, 128], replicated
- query_mask: int32 [512, 32], P(('replica', 'data2', 'data'))
- doc_mask: int32 [512, 512], P(('replica', 'data2', 'data'))
- temperature: float32 [], replicated
Outputs:
- output 1: float32 [512], P(('replica', 'data2', 'data'))
- output 2: float32 [1], P('replica')
All inputs are finite; a program needn't handle non-finite values.
Results may differ from the reference program's by a relative error of at most 0.001.
Values are sent between devices in bfloat16 or wider.
A program may use at most 1 GiB of HBM per device.

```python
import jax
import jax.numpy as jnp
from jax import lax

BATCH = 512
QLEN = 32
DLEN = 512
HIDDEN = 768
PROJ = 128


def setup_inputs(seed: int = 0, part: int = 0) -> dict:
    root_key = jax.random.key(seed)
    key_common, key_parts = jax.random.split(root_key)
    part_key = jax.random.fold_in(key_parts, part)
    key_list = jax.random.split(part_key, 6)
    key_weight, key_temp = jax.random.split(key_common)
    shared = jax.random.normal(key_list[0], (HIDDEN,), jnp.float32)
    topic_vec = jax.random.normal(key_list[1], (BATCH, 1, HIDDEN), jnp.float32)
    concept = jax.random.normal(key_list[2], (BATCH, QLEN, HIDDEN), jnp.float32)
    token_noise = jax.random.normal(key_list[3], (BATCH, DLEN, HIDDEN), jnp.float32)
    query_lens = jax.random.randint(key_list[4], (BATCH,), QLEN // 2, QLEN + 1)
    doc_lens = jax.random.randint(key_list[5], (BATCH,), DLEN // 4, DLEN + 1)
    query_mask = (jnp.arange(QLEN)[None, :] < query_lens[:, None]).astype(jnp.int32)
    doc_mask = (jnp.arange(DLEN)[None, :] < doc_lens[:, None]).astype(jnp.int32)
    base_state = 0.6 * shared + 0.6 * topic_vec
    query_hidden = base_state + concept
    doc_concept = jnp.take(concept, jnp.arange(DLEN) % QLEN, axis=1)
    real_tok = base_state + 0.6 * doc_concept + 0.8 * token_noise
    pad_tok = 1.5 * shared + token_noise
    doc_hidden = jnp.where(doc_mask[:, :, None] > 0, real_tok, pad_tok)
    w_proj = jax.random.normal(key_weight, (HIDDEN, PROJ), jnp.float32) * HIDDEN ** -0.5
    temperature = QLEN * jax.random.uniform(key_temp, (), jnp.float32, 0.8, 1.25) / 8.0
    return {'query_hidden': query_hidden.astype(jnp.bfloat16), 'doc_hidden': doc_hidden.astype(jnp.bfloat16), 'w_proj': w_proj.astype(jnp.bfloat16), 'query_mask': query_mask, 'doc_mask': doc_mask, 'temperature': temperature}


def project_norm(hidden, w_proj):
    flat_states = hidden.reshape(-1, HIDDEN)
    projected = jnp.dot(flat_states, w_proj, preferred_element_type=jnp.float32)
    norm_len = jnp.sqrt(jnp.sum(projected * projected, axis=-1, keepdims=True))
    unit_vecs = projected / jnp.maximum(norm_len, 1e-12)
    return unit_vecs.astype(jnp.bfloat16).reshape(hidden.shape[0], hidden.shape[1], PROJ)


def reference(query_hidden, doc_hidden, w_proj, query_mask, doc_mask, temperature):
    q_vecs = project_norm(query_hidden, w_proj)
    p_vecs = project_norm(doc_hidden, w_proj).astype(jnp.float32)
    doc_valid = doc_mask[None, :, :] > 0

    def query_row(query_args):
        q_tok, q_weight = query_args
        similarity = jnp.einsum('tc,jsc->tjs', q_tok.astype(jnp.float32), p_vecs)
        best_match = jnp.max(jnp.where(doc_valid, similarity, -jnp.inf), axis=-1)
        return jnp.sum(q_weight.astype(jnp.float32)[:, None] * best_match, axis=0)

    scores = lax.map(query_row, (q_vecs, query_mask))
    logits = scores / temperature
    losses = jax.nn.logsumexp(logits, axis=1) - jnp.diagonal(logits)
    mean_loss = jnp.mean(losses).reshape(1)
    return losses, mean_loss
```

```python
import jax
import jax.numpy as jnp
from jax import lax
from jax.experimental import pallas as pl
from jax.experimental.pallas import tpu as pltpu
from jax.sharding import PartitionSpec as P

MESH = pl.DeviceIdType.MESH
NQ, LQ, LD, HID, DIM = 4, 32, 512, 768, 128
SIDE = 4
TOTAL = 512
ORDERS = (('x', 'y', 'z'), ('y', 'z', 'x'), ('z', 'x', 'y'), ('x', 'z', 'y'))


def unit_rows(projected):
    square = jnp.sum(projected * projected, axis=-1, keepdims=True)
    return projected * jnp.minimum(lax.rsqrt(square), 1e12)


def kernel(qh_hbm, dh_hbm, w_hbm, qm_hbm, dm_hbm, temp_hbm, loss_ref, mean_ref,
           qh, dh, w, qm, dm, temp, qbuf, pbuf, sacc, xbuf, ybuf, zbuf,
           in_sem, send_sem, recv_sem):
    outer, inner = lax.axis_index('data2'), lax.axis_index('data')
    here = {'z': outer // SIDE, 'y': outer % SIDE, 'x': inner // 2}
    core = inner % 2

    def moved(axis, step, same_core=True):
        at = dict(here)
        at[axis] = (here[axis] + step) % SIDE
        c = core if same_core else 1 - core
        return {'data2': at['z'] * SIDE + at['y'], 'data': at['x'] * 2 + c}

    sibling = moved('x', 0, False)
    used = [0]
    sent = []

    def message():
        used[0] += 1
        return used[0] - 1

    def push(slot, src, dst, device):
        copy = pltpu.make_async_remote_copy(src_ref=src, dst_ref=dst, send_sem=send_sem.at[slot],
                                            recv_sem=recv_sem.at[slot], device_id=device, device_id_type=MESH)
        copy.start()
        sent.append(copy)

    def arrived(slot, dst):
        pltpu.make_async_remote_copy(src_ref=dst, dst_ref=dst, send_sem=send_sem.at[slot],
                                     recv_sem=recv_sem.at[slot], device_id=sibling, device_id_type=MESH).wait_recv()

    loads = [pltpu.make_async_copy(s, d, in_sem.at[i]) for i, (s, d) in enumerate(
        [(w_hbm, w), (qh_hbm, qh), (qm_hbm, qm), (dm_hbm, dm), (temp_hbm, temp)]
        + [(dh_hbm.at[d], dh.at[d]) for d in range(NQ)])]
    for load in loads:
        load.start()

    partners = [moved(a, s) for a in ('x', 'y', 'z') for s in (1, 2, 3)] + [moved('z', s, False) for s in range(SIDE)]
    barrier = pltpu.get_barrier_semaphore()
    for device in partners:
        pl.semaphore_signal(barrier, inc=1, device_id=device, device_id_type=MESH)

    def coords(o):
        return [here[a] for a in ORDERS[o]]

    def row_of(o, r3, r2):
        c1, c2, c3 = coords(o)
        return ((c3 + r3) % SIDE) * SIDE + (c2 + r2) % SIDE

    def row(o, r3, r2):
        return qbuf.at[o, row_of(o, r3, r2)]

    def block(o, r1):
        c1 = coords(o)[0]
        start = pl.multiple_of(((c1 + r1) % SIDE) * LQ, LQ)
        return qbuf.at[o, row_of(o, 0, 0), pl.ds(start, LQ)]

    loads[0].wait()
    loads[1].wait()
    loads[2].wait()
    mask_t = jnp.transpose(jnp.concatenate(
        [jnp.concatenate([qm[...].astype(jnp.float32), jnp.zeros((NQ, DIM - LQ), jnp.float32)], axis=1),
         jnp.zeros((8 - NQ, DIM), jnp.float32)], axis=0))
    for o in range(NQ):
        q = unit_rows(jnp.dot(qh[pl.ds(o * LQ, LQ)], w[...], preferred_element_type=jnp.float32))
        keep = mask_t[:LQ, o:o + 1] > 0
        block(o, 0)[...] = jnp.where(keep, q, 0.0).astype(jnp.bfloat16)
    sacc[...] = jnp.zeros_like(sacc)

    pl.semaphore_wait(barrier, len(partners))

    m1 = {(o, s): message() for o in range(NQ) for s in (1, 2, 3)}
    m2 = {(o, s): message() for o in range(NQ) for s in (1, 2, 3)}
    m3 = {(o, s, r): message() for o in range(NQ) for s in (1, 3) for r in range(SIDE)}
    m4 = {(o, r): message() for o in range(NQ) for r in range(SIDE)}
    mp = [message() for _ in range(NQ)]
    mx = {s: message() for s in (1, 2, 3)}
    my = {s: message() for s in (1, 2, 3)}
    mz = {(s, same): message() for s in range(SIDE) for same in (True, False) if s or not same}

    for s in (1, 3, 2):
        for o in range(NQ):
            push(m1[o, s], block(o, 0), block(o, 0), moved(ORDERS[o][0], s))

    loads[3].wait()
    valid = dm[...].astype(jnp.float32)
    key = valid * (LD - lax.broadcasted_iota(jnp.int32, (NQ, LD), 1)).astype(jnp.float32)
    key_t = jnp.transpose(jnp.concatenate([key, jnp.zeros((8 - NQ, LD), jnp.float32)], axis=0))
    for d in range(NQ):
        loads[5 + d].wait()
        p = unit_rows(jnp.dot(dh[d], w[...], preferred_element_type=jnp.float32))
        col = key_t[:, d:d + 1]
        first = jnp.max(col, axis=0, keepdims=True)
        colb = jnp.broadcast_to(col, (LD, DIM))
        stand_in = jnp.sum(jnp.where(colb == first, p, 0.0), axis=0, keepdims=True)
        pbuf[d] = jnp.where(colb > 0, p, stand_in).astype(jnp.bfloat16)
        push(mp[d], pbuf.at[d], pbuf.at[NQ + d], sibling)

    lane = lax.broadcasted_iota(jnp.int32, (8, DIM), 1)

    def score(units):
        for u, v in zip(units[::2], units[1::2]):
            q = jnp.concatenate([row(*u)[...], row(*v)[...]], axis=0)
            best = []
            for d in range(2 * NQ):
                sim = lax.dot_general(pbuf[d], q, (((1,), (1,)), ((), ())), preferred_element_type=jnp.float32)
                peak = jnp.max(sim.reshape(LD // 8, 8, 2 * DIM), axis=0)
                best.append(jnp.max(peak, axis=0, keepdims=True))
            best = jnp.concatenate(best, axis=0)
            for i, (o, r3, r2) in enumerate((u, v)):
                t = best[:, i * DIM:(i + 1) * DIM]
                for shift in (16, 8, 4, 2, 1):
                    t = t + pltpu.roll(t, DIM - shift, 1)
                place = (o % 2) * 16 + row_of(o, r3, r2)
                t = pltpu.roll(t, place, 1)
                sacc[o // 2] = jnp.where(lane % LQ == place, t, sacc[o // 2])

    def rows(*which):
        return [(o, r3, r2) for r3, r2 in which for o in range(NQ)]

    for o in range(NQ):
        for s in (1, 3, 2):
            arrived(m1[o, s], block(o, -s))
        for s in (1, 3, 2):
            push(m2[o, s], row(o, 0, 0), row(o, 0, 0), moved(ORDERS[o][1], s))
        for s in (1, 3):
            push(m3[o, s, 0], row(o, 0, 0), row(o, 0, 0), moved(ORDERS[o][2], s))
    for d in range(NQ):
        arrived(mp[d], pbuf.at[NQ + d])
    score(rows((0, 0)))

    def second(o, s):
        r = -s % SIDE
        arrived(m2[o, s], row(o, 0, r))
        for t in (1, 3):
            push(m3[o, t, r], row(o, 0, r), row(o, 0, r), moved(ORDERS[o][2], t))

    def third(o, s, r, forward):
        arrived(m3[o, s, r], row(o, -s, r))
        if forward:
            push(m4[o, r], row(o, -s, r), row(o, -s, r), moved(ORDERS[o][2], s))

    for o in range(NQ):
        second(o, 1)
        second(o, 3)
    score(rows((0, 1), (0, 3)))
    for o in range(NQ):
        second(o, 2)
    for o in range(NQ):
        third(o, 1, 0, True)
        third(o, 3, 0, False)
    score(rows((1, 0), (3, 0)))
    for o in range(NQ):
        third(o, 1, 1, True)
        third(o, 3, 3, True)
    for o in range(NQ):
        third(o, 1, 3, False)
        third(o, 3, 1, False)
    score(rows((0, 2), (1, 1)))
    for o in range(NQ):
        third(o, 3, 2, True)
        third(o, 1, 2, False)
    score(rows((1, 3), (3, 1)))
    score(rows((3, 3), (1, 2)))
    for o in range(NQ):
        arrived(m4[o, 0], row(o, 2, 0))
    score(rows((3, 2), (2, 0)))
    for o in range(NQ):
        arrived(m4[o, 1], row(o, 2, 1))
        arrived(m4[o, 3], row(o, 2, 3))
    score(rows((2, 1), (2, 3)))
    for o in range(NQ):
        arrived(m4[o, 2], row(o, 2, 2))
    score(rows((2, 2)))

    loads[4].wait()
    lane1 = lane[:1]
    sub = lax.broadcasted_iota(jnp.int32, (8, DIM), 0)

    def own_lane(o):
        c1, c2, c3 = coords(o)
        return c1 * LQ + (o % 2) * 16 + c3 * SIDE + c2

    tops, sums, positives = [], [], []
    for g in range(2):
        logit = sacc[g] / temp[0]
        top = jnp.max(logit, axis=0, keepdims=True)
        tops.append(top)
        sums.append(jnp.sum(jnp.exp(logit - top), axis=0, keepdims=True))
        mine = jnp.zeros((8, DIM), jnp.float32)
        for o in (2 * g, 2 * g + 1):
            mine = jnp.where((sub == o) & (lane == own_lane(o)), logit, mine)
        positives.append(jnp.sum(mine, axis=0, keepdims=True))
    part = jnp.concatenate(tops + sums + positives + [jnp.zeros((2, DIM), jnp.float32)], axis=0)

    def merge(parts):
        top = jnp.maximum(jnp.maximum(parts[0][0:2], parts[1][0:2]), jnp.maximum(parts[2][0:2], parts[3][0:2]))
        total = sum(p[2:4] * jnp.exp(p[0:2] - top) for p in parts)
        positive = sum(p[4:6] for p in parts)
        return top, total, positive

    def packed(top, total, positive):
        return jnp.concatenate([top, total, positive, jnp.zeros((2, DIM), jnp.float32)], axis=0)

    for axis, buf, slots in (('x', xbuf, mx), ('y', ybuf, my)):
        at = here[axis]
        buf[at] = part
        for s in (2, 1, 3):
            push(slots[s], buf.at[at], buf.at[at], moved(axis, s))
        for s in (1, 3, 2):
            arrived(slots[s], buf.at[(at - s) % SIDE])
        part = packed(*merge([buf[i] for i in range(SIDE)]))
    at = here['z']
    zbuf[core * SIDE + at] = part
    for s in (2, 1, 3, 0):
        for same in (True, False):
            if s or not same:
                push(mz[s, same], zbuf.at[core * SIDE + at], zbuf.at[core * SIDE + at], moved('z', s, same))
    for s in (0, 1, 3, 2):
        for same in (True, False):
            if s or not same:
                other = core if same else 1 - core
                arrived(mz[s, same], zbuf.at[other * SIDE + (at - s) % SIDE])
    total_loss = jnp.zeros((1, 1), jnp.float32)
    for c in range(2):
        top, total, positive = merge([zbuf[c * SIDE + i] for i in range(SIDE)])
        loss = top + jnp.log(total) - positive
        total_loss = total_loss + jnp.sum(jnp.sum(loss, axis=0, keepdims=True), axis=1, keepdims=True)
        if c == 0:
            losses = loss
        else:
            losses = jnp.where(core == 0, losses, loss)
    mean_ref[...] = total_loss / TOTAL
    row_loss = jnp.zeros((1, DIM), jnp.float32)
    for o in range(NQ):
        g = o // 2
        value = jnp.sum(jnp.where(lane1 == own_lane(o), losses[g:g + 1], 0.0), axis=1, keepdims=True)
        row_loss = jnp.where(lane1 == o, value, row_loss)
    loss_ref[...] = row_loss[:, :NQ]

    for copy in sent:
        copy.wait_send()


def solution(mesh):
    row_spec = P(('replica', 'data2', 'data'))
    tok_spec = P(('replica', 'data2', 'data'), None, None)
    mask_spec = P(('replica', 'data2', 'data'), None)
    n_msg = 12 + 12 + 32 + 16 + 4 + 3 + 3 + 7

    def local_step(query_hidden, doc_hidden, w_proj, query_mask, doc_mask, temperature):
        losses, mean = pl.pallas_call(
            kernel,
            out_shape=(jax.ShapeDtypeStruct((1, NQ), jnp.float32), jax.ShapeDtypeStruct((1, 1), jnp.float32)),
            in_specs=[pl.BlockSpec(memory_space=pl.ANY)] * 6,
            out_specs=(pl.BlockSpec(memory_space=pltpu.VMEM), pl.BlockSpec(memory_space=pltpu.VMEM)),
            scratch_shapes=[
                pltpu.VMEM((NQ * LQ, HID), jnp.bfloat16),
                pltpu.VMEM((NQ, LD, HID), jnp.bfloat16),
                pltpu.VMEM((HID, DIM), jnp.bfloat16),
                pltpu.VMEM((NQ, LQ), jnp.int32),
                pltpu.VMEM((NQ, LD), jnp.int32),
                pltpu.SMEM((1,), jnp.float32),
                pltpu.VMEM((NQ, SIDE * SIDE, SIDE * LQ, DIM), jnp.bfloat16),
                pltpu.VMEM((2 * NQ, LD, DIM), jnp.bfloat16),
                pltpu.VMEM((2, 8, DIM), jnp.float32),
                pltpu.VMEM((SIDE, 8, DIM), jnp.float32),
                pltpu.VMEM((SIDE, 8, DIM), jnp.float32),
                pltpu.VMEM((2 * SIDE, 8, DIM), jnp.float32),
                pltpu.SemaphoreType.DMA((9,)),
                pltpu.SemaphoreType.DMA((n_msg,)),
                pltpu.SemaphoreType.DMA((n_msg,)),
            ],
            compiler_params=pltpu.CompilerParams(collective_id=0, has_side_effects=True, vmem_limit_bytes=48 << 20),
            name='late_interaction_loss',
        )(query_hidden.reshape(NQ * LQ, HID), doc_hidden, w_proj, query_mask, doc_mask, temperature.reshape(1))
        return losses.reshape(NQ), mean.reshape(1)

    return jax.shard_map(local_step, mesh=mesh, in_specs=(tok_spec, tok_spec, P(None, None), mask_spec, mask_spec, P()),
                         out_specs=(row_spec, P('replica')), check_vma=False)
```

```python
import functools

import jax
import jax.numpy as jnp
from jax import lax
from jax.experimental import pallas as pl
from jax.experimental.pallas import tpu as pltpu
from jax.sharding import PartitionSpec as P

MESH = pl.DeviceIdType.MESH
NQ, LQ, LD, HID, DIM = 4, 32, 512, 768, 128
SIDE = 4
TOTAL = 512
ORDERS = (('x', 'y', 'z'), ('y', 'z', 'x'), ('z', 'x', 'y'), ('x', 'z', 'y'))


def unit_rows(projected):
    square = jnp.sum(projected * projected, axis=-1, keepdims=True)
    return projected * jnp.minimum(lax.rsqrt(square), 1e12)


def kernel(qh_hbm, dh_hbm, w_hbm, qm_hbm, dm_hbm, temp_hbm, out_ref,
           qh, dh, w, qm, dm, temp, qbuf, pbuf, sacc, xybuf, zbuf,
           in_sem, send_sem, recv_sem):
    outer, inner = lax.axis_index('data2'), lax.axis_index('data')
    here = {'z': outer // SIDE, 'y': outer % SIDE, 'x': inner // 2}
    core = inner % 2

    def moved(axis, step, same_core=True, axis2='x', step2=0):
        at = dict(here)
        at[axis] = (at[axis] + step) % SIDE
        at[axis2] = (at[axis2] + step2) % SIDE
        c = core if same_core else 1 - core
        return {'data2': at['z'] * SIDE + at['y'], 'data': at['x'] * 2 + c}

    sibling = moved('x', 0, False)
    used = [0]
    sent = []

    def message():
        used[0] += 1
        return used[0] - 1

    def push(slot, src, dst, device):
        copy = pltpu.make_async_remote_copy(src_ref=src, dst_ref=dst, send_sem=send_sem.at[slot],
                                            recv_sem=recv_sem.at[slot], device_id=device, device_id_type=MESH)
        copy.start()
        sent.append(copy)

    def arrived(slot, dst):
        pltpu.make_async_remote_copy(src_ref=dst, dst_ref=dst, send_sem=send_sem.at[slot],
                                     recv_sem=recv_sem.at[slot], device_id=sibling, device_id_type=MESH).wait_recv()

    loads = [pltpu.make_async_copy(s, d, in_sem.at[i]) for i, (s, d) in enumerate(
        [(w_hbm, w), (qh_hbm, qh), (qm_hbm, qm), (dm_hbm, dm), (temp_hbm, temp)]
        + [(dh_hbm.at[d], dh.at[d]) for d in range(NQ)])]
    for load in loads:
        load.start()

    partners = [moved(a, s) for a in ('x', 'y', 'z') for s in (1, 2, 3)] + [moved('z', s, False) for s in range(SIDE)]
    barrier = pltpu.get_barrier_semaphore()
    for device in partners:
        pl.semaphore_signal(barrier, inc=1, device_id=device, device_id_type=MESH)

    def coords(o):
        return [here[a] for a in ORDERS[o]]

    def row_of(o, r3, r2):
        c1, c2, c3 = coords(o)
        return ((c3 + r3) % SIDE) * SIDE + (c2 + r2) % SIDE

    def row(o, r3, r2):
        return qbuf.at[o, row_of(o, r3, r2)]

    def block(o, r1):
        c1 = coords(o)[0]
        start = pl.multiple_of(((c1 + r1) % SIDE) * LQ, LQ)
        return qbuf.at[o, row_of(o, 0, 0), pl.ds(start, LQ)]

    loads[0].wait()
    loads[1].wait()
    loads[2].wait()
    mask_t = jnp.transpose(jnp.concatenate(
        [jnp.concatenate([qm[...].astype(jnp.float32), jnp.zeros((NQ, DIM - LQ), jnp.float32)], axis=1),
         jnp.zeros((8 - NQ, DIM), jnp.float32)], axis=0))
    q = unit_rows(jnp.dot(qh[...], w[...], preferred_element_type=jnp.float32))
    for o in range(NQ):
        keep = mask_t[:LQ, o:o + 1] > 0
        block(o, 0)[...] = jnp.where(keep, q[o * LQ:(o + 1) * LQ], 0.0).astype(jnp.bfloat16)
    sacc[...] = jnp.zeros_like(sacc)

    m1 = {(o, s): message() for o in range(NQ) for s in (1, 2, 3)}
    m2 = {(o, s): message() for o in range(NQ) for s in (1, 2, 3)}
    m3 = {(o, s, r): message() for o in range(NQ) for s in (1, 3) for r in range(SIDE)}
    m4 = {(o, r): message() for o in range(NQ) for r in range(SIDE)}
    mp = [message() for _ in range(NQ)]
    mxy = {(sx, sy): message() for sx in range(SIDE) for sy in range(SIDE) if sx or sy}
    mz = {(s, same): message() for s in range(SIDE) for same in (True, False) if s or not same}

    loads[3].wait()
    valid = dm[...].astype(jnp.float32)
    key = valid * (LD - lax.broadcasted_iota(jnp.int32, (NQ, LD), 1)).astype(jnp.float32)
    key_t = jnp.transpose(jnp.concatenate([key, jnp.zeros((8 - NQ, LD), jnp.float32)], axis=0))

    def project(docs):
        for d in docs:
            loads[5 + d].wait()
        for d in docs:
            project_one(d)

    def project_one(d):
        p = unit_rows(jnp.dot(dh[d], w[...], preferred_element_type=jnp.float32))
        col = key_t[:, d:d + 1]
        first = jnp.max(col, axis=0, keepdims=True)
        colb = jnp.broadcast_to(col, (LD, DIM))
        stand_in = jnp.sum(jnp.where(colb == first, p, 0.0), axis=0, keepdims=True)
        pbuf[d] = jnp.where(colb > 0, p, stand_in).astype(jnp.bfloat16)

    project((0, 1))
    pl.semaphore_wait(barrier, len(partners))

    for s in (1, 3, 2):
        for o in range(NQ):
            push(m1[o, s], block(o, 0), block(o, 0), moved(ORDERS[o][0], s))

    for d in (0, 1):
        push(mp[d], pbuf.at[d], pbuf.at[NQ + d], sibling)
    project((2, 3))
    for d in (2, 3):
        push(mp[d], pbuf.at[d], pbuf.at[NQ + d], sibling)

    lane = lax.broadcasted_iota(jnp.int32, (8, DIM), 1)

    def score(units):
        for u, v in zip(units[::2], units[1::2]):
            q = jnp.concatenate([row(*u)[...], row(*v)[...]], axis=0)
            best = []
            for d in range(2 * NQ):
                sim = lax.dot_general(pbuf[d], q, (((1,), (1,)), ((), ())), preferred_element_type=jnp.float32)
                peak = jnp.max(sim.reshape(LD // 8, 8, 2 * DIM), axis=0)
                best.append(jnp.max(peak, axis=0, keepdims=True))
            best = jnp.concatenate(best, axis=0)
            for i, (o, r3, r2) in enumerate((u, v)):
                t = best[:, i * DIM:(i + 1) * DIM]
                for shift in (16, 8, 4, 2, 1):
                    t = t + pltpu.roll(t, DIM - shift, 1)
                place = (o % 2) * 16 + row_of(o, r3, r2)
                t = pltpu.roll(t, place, 1)
                sacc[o // 2] = jnp.where(lane % LQ == place, t, sacc[o // 2])

    def rows(*which):
        return [(o, r3, r2) for r3, r2 in which for o in range(NQ)]

    for o in range(NQ):
        for s in (1, 3, 2):
            arrived(m1[o, s], block(o, -s))
        for s in (1, 3):
            push(m2[o, s], row(o, 0, 0), row(o, 0, 0), moved(ORDERS[o][1], s))
    for o in range(NQ):
        for s in (1, 3):
            push(m3[o, s, 0], row(o, 0, 0), row(o, 0, 0), moved(ORDERS[o][2], s))
    for d in range(NQ):
        arrived(mp[d], pbuf.at[NQ + d])
    score(rows((0, 0)))
    for o in range(NQ):
        push(m2[o, 2], row(o, 0, 0), row(o, 0, 0), moved(ORDERS[o][1], 2))

    def second(o, s):
        r = -s % SIDE
        arrived(m2[o, s], row(o, 0, r))
        for t in (1, 3):
            push(m3[o, t, r], row(o, 0, r), row(o, 0, r), moved(ORDERS[o][2], t))

    def third(o, s, r, forward):
        arrived(m3[o, s, r], row(o, -s, r))
        if forward:
            push(m4[o, r], row(o, -s, r), row(o, -s, r), moved(ORDERS[o][2], s))

    for o in range(NQ):
        second(o, 1)
        second(o, 3)
    score(rows((0, 1), (0, 3)))
    for o in range(NQ):
        third(o, 1, 0, True)
        third(o, 3, 0, False)
    for o in range(NQ):
        second(o, 2)
    score(rows((1, 0), (3, 0)))
    for o in range(NQ):
        third(o, 1, 1, True)
        third(o, 3, 3, True)
    for o in range(NQ):
        third(o, 1, 3, False)
        third(o, 3, 1, False)
    score(rows((0, 2), (1, 1)))
    for o in range(NQ):
        third(o, 3, 2, True)
        third(o, 1, 2, False)
    score(rows((1, 3), (3, 1), (3, 3), (1, 2)))
    for o in range(NQ):
        arrived(m4[o, 0], row(o, 2, 0))
        arrived(m4[o, 1], row(o, 2, 1))
        arrived(m4[o, 3], row(o, 2, 3))
    score(rows((3, 2), (2, 0), (2, 1), (2, 3)))
    for o in range(NQ):
        arrived(m4[o, 2], row(o, 2, 2))
    score(rows((2, 2)))

    loads[4].wait()
    lane1 = lane[:1]
    sub = lax.broadcasted_iota(jnp.int32, (8, DIM), 0)

    def own_lane(o):
        c1, c2, c3 = coords(o)
        return c1 * LQ + (o % 2) * 16 + c3 * SIDE + c2

    tops, sums, positives = [], [], []
    for g in range(2):
        logit = sacc[g] / temp[0]
        top = jnp.max(logit, axis=0, keepdims=True)
        tops.append(top)
        sums.append(jnp.sum(jnp.exp(logit - top), axis=0, keepdims=True))
        mine = jnp.zeros((8, DIM), jnp.float32)
        for o in (2 * g, 2 * g + 1):
            mine = jnp.where((sub == o) & (lane == own_lane(o)), logit, mine)
        positives.append(jnp.sum(mine, axis=0, keepdims=True))
    part = jnp.concatenate(tops + sums + positives + [jnp.zeros((2, DIM), jnp.float32)], axis=0)

    def merge(parts):
        top = functools.reduce(jnp.maximum, [p[0:2] for p in parts])
        total = sum(p[2:4] * jnp.exp(p[0:2] - top) for p in parts)
        positive = sum(p[4:6] for p in parts)
        return top, total, positive

    at = here['y'] * SIDE + here['x']
    xybuf[at] = part
    plane = [(sx, sy) for sy in (2, 1, 3, 0) for sx in (2, 1, 3, 0) if sx or sy]
    for sx, sy in plane:
        push(mxy[sx, sy], xybuf.at[at], xybuf.at[at], moved('x', sx, True, 'y', sy))
    for sx, sy in plane[::-1]:
        arrived(mxy[sx, sy], xybuf.at[((here['y'] - sy) % SIDE) * SIDE + (here['x'] - sx) % SIDE])
    part = jnp.concatenate([*merge([xybuf[i] for i in range(SIDE * SIDE)]), jnp.zeros((2, DIM), jnp.float32)], axis=0)
    at = here['z']
    zbuf[core * SIDE + at] = part
    for s in (2, 1, 3, 0):
        for same in (True, False):
            if s or not same:
                push(mz[s, same], zbuf.at[core * SIDE + at], zbuf.at[core * SIDE + at], moved('z', s, same))
    for s in (0, 1, 3, 2):
        for same in (True, False):
            if s or not same:
                other = core if same else 1 - core
                arrived(mz[s, same], zbuf.at[other * SIDE + (at - s) % SIDE])
    total_loss = jnp.zeros((1, 1), jnp.float32)
    for c in range(2):
        top, total, positive = merge([zbuf[c * SIDE + i] for i in range(SIDE)])
        loss = top + jnp.log(total) - positive
        total_loss = total_loss + jnp.sum(jnp.sum(loss, axis=0, keepdims=True), axis=1, keepdims=True)
        if c == 0:
            losses = loss
        else:
            losses = jnp.where(core == 0, losses, loss)
    row_loss = jnp.zeros((1, DIM), jnp.float32)
    for o in range(NQ):
        g = o // 2
        value = jnp.sum(jnp.where(lane1 == own_lane(o), losses[g:g + 1], 0.0), axis=1, keepdims=True)
        row_loss = jnp.where(lane1 == o, value, row_loss)
    out_ref[...] = jnp.concatenate([row_loss, jnp.broadcast_to(total_loss / TOTAL, (7, DIM))], axis=0)

    for copy in sent:
        copy.wait_send()


def split_result(out_ref, loss_ref, mean_ref):
    loss_ref[...] = out_ref[0, :NQ]
    mean_ref[...] = out_ref[1, :1]


def solution(mesh):
    row_spec = P(('replica', 'data2', 'data'))
    tok_spec = P(('replica', 'data2', 'data'), None, None)
    mask_spec = P(('replica', 'data2', 'data'), None)
    n_msg = 12 + 12 + 32 + 16 + 4 + 15 + 7

    def local_step(query_hidden, doc_hidden, w_proj, query_mask, doc_mask, temperature):
        out = pl.pallas_call(
            kernel,
            out_shape=jax.ShapeDtypeStruct((8, DIM), jnp.float32),
            in_specs=[pl.BlockSpec(memory_space=pltpu.HBM)] * 6,
            out_specs=pl.BlockSpec(memory_space=pltpu.VMEM),
            scratch_shapes=[
                pltpu.VMEM((NQ * LQ, HID), jnp.bfloat16),
                pltpu.VMEM((NQ, LD, HID), jnp.bfloat16),
                pltpu.VMEM((HID, DIM), jnp.bfloat16),
                pltpu.VMEM((NQ, LQ), jnp.int32),
                pltpu.VMEM((NQ, LD), jnp.int32),
                pltpu.SMEM((1,), jnp.float32),
                pltpu.VMEM((NQ, SIDE * SIDE, SIDE * LQ, DIM), jnp.bfloat16),
                pltpu.VMEM((2 * NQ, LD, DIM), jnp.bfloat16),
                pltpu.VMEM((2, 8, DIM), jnp.float32),
                pltpu.VMEM((SIDE * SIDE, 8, DIM), jnp.float32),
                pltpu.VMEM((2 * SIDE, 8, DIM), jnp.float32),
                pltpu.SemaphoreType.DMA((9,)),
                pltpu.SemaphoreType.DMA((n_msg,)),
                pltpu.SemaphoreType.DMA((n_msg,)),
            ],
            compiler_params=pltpu.CompilerParams(collective_id=0, has_side_effects=True, vmem_limit_bytes=67043328),
            name='late_interaction_loss',
        )(query_hidden.reshape(NQ * LQ, HID), doc_hidden, w_proj, query_mask, doc_mask, temperature.reshape(1))
        losses, mean = pl.pallas_call(
            split_result,
            out_shape=(jax.ShapeDtypeStruct((NQ,), jnp.float32), jax.ShapeDtypeStruct((1,), jnp.float32)),
            in_specs=[pl.BlockSpec(memory_space=pltpu.VMEM)],
            out_specs=(pl.BlockSpec(memory_space=pltpu.VMEM), pl.BlockSpec(memory_space=pltpu.VMEM)),
            name='split_result',
        )(out)
        return losses, mean

    return jax.shard_map(local_step, mesh=mesh, in_specs=(tok_spec, tok_spec, P(None, None), mask_spec, mask_spec, P()),
                         out_specs=(row_spec, P('replica')), check_vma=False)
```

```python
import functools

import jax
import jax.numpy as jnp
from jax import lax
from jax.experimental import pallas as pl
from jax.experimental.pallas import tpu as pltpu
from jax.sharding import PartitionSpec as P

MESH = pl.DeviceIdType.MESH
NQ, LQ, LD, HID, DIM = 4, 32, 512, 768, 128
SIDE = 4
TOTAL = 512
ORDERS = (('x', 'y', 'z'), ('y', 'z', 'x'), ('z', 'x', 'y'), ('z', 'y', 'x'))


def unit_rows(projected):
    square = jnp.sum(projected * projected, axis=-1, keepdims=True)
    return projected * jnp.minimum(lax.rsqrt(square), 1e12)


def kernel(qh_hbm, dh_hbm, w_hbm, qm_hbm, dm_hbm, temp_hbm, out_ref,
           qh, dh, w, qm, dm, temp, qbuf, pbuf, sacc, xybuf, zbuf,
           in_sem, send_sem, recv_sem):
    outer, inner = lax.axis_index('data2'), lax.axis_index('data')
    here = {'z': outer // SIDE, 'y': outer % SIDE, 'x': inner // 2}
    core = inner % 2

    def moved(axis, step, same_core=True, axis2='x', step2=0):
        at = dict(here)
        at[axis] = (at[axis] + step) % SIDE
        at[axis2] = (at[axis2] + step2) % SIDE
        c = core if same_core else 1 - core
        return {'data2': at['z'] * SIDE + at['y'], 'data': at['x'] * 2 + c}

    sibling = moved('x', 0, False)
    used = [0]
    sent = []

    def message():
        used[0] += 1
        return used[0] - 1

    def push(slot, src, dst, device):
        copy = pltpu.make_async_remote_copy(src_ref=src, dst_ref=dst, send_sem=send_sem.at[slot],
                                            recv_sem=recv_sem.at[slot], device_id=device, device_id_type=MESH)
        copy.start()
        sent.append(copy)

    def arrived(slot, dst):
        pltpu.make_async_remote_copy(src_ref=dst, dst_ref=dst, send_sem=send_sem.at[slot],
                                     recv_sem=recv_sem.at[slot], device_id=sibling, device_id_type=MESH).wait_recv()

    loads = [pltpu.make_async_copy(s, d, in_sem.at[i]) for i, (s, d) in enumerate(
        [(w_hbm, w), (qh_hbm, qh), (qm_hbm, qm), (dm_hbm, dm), (temp_hbm, temp)]
        + [(dh_hbm.at[d], dh.at[d]) for d in range(NQ)])]
    for load in loads:
        load.start()

    partners = [moved(a, s) for a in ('x', 'y', 'z') for s in (1, 2, 3)] + [moved('z', s, False) for s in range(SIDE)]
    barrier = pltpu.get_barrier_semaphore()
    for device in partners:
        pl.semaphore_signal(barrier, inc=1, device_id=device, device_id_type=MESH)

    def coords(o):
        return [here[a] for a in ORDERS[o]]

    def row_of(o, r3, r2):
        c1, c2, c3 = coords(o)
        return ((c3 + r3) % SIDE) * SIDE + (c2 + r2) % SIDE

    def row(o, r3, r2):
        return qbuf.at[o, row_of(o, r3, r2)]

    def block(o, r1):
        c1 = coords(o)[0]
        start = pl.multiple_of(((c1 + r1) % SIDE) * LQ, LQ)
        return qbuf.at[o, row_of(o, 0, 0), pl.ds(start, LQ)]

    loads[0].wait()
    loads[1].wait()
    loads[2].wait()
    mask_t = jnp.transpose(jnp.concatenate(
        [jnp.concatenate([qm[...].astype(jnp.float32), jnp.zeros((NQ, DIM - LQ), jnp.float32)], axis=1),
         jnp.zeros((8 - NQ, DIM), jnp.float32)], axis=0))
    q = unit_rows(jnp.dot(qh[...], w[...], preferred_element_type=jnp.float32))
    for o in range(NQ):
        keep = mask_t[:LQ, o:o + 1] > 0
        block(o, 0)[...] = jnp.where(keep, q[o * LQ:(o + 1) * LQ], 0.0).astype(jnp.bfloat16)
    sacc[...] = jnp.zeros_like(sacc)

    m1 = {(o, s): message() for o in range(NQ) for s in (1, 2, 3)}
    m2 = {(o, s): message() for o in range(NQ) for s in (1, 2, 3)}
    m3 = {(o, s, r): message() for o in range(NQ) for s in (1, 3) for r in range(SIDE)}
    m4 = {(o, r): message() for o in range(NQ) for r in range(SIDE)}
    mp = [message() for _ in range(NQ)]
    mxy = {(sx, sy): message() for sx in range(SIDE) for sy in range(SIDE) if sx or sy}
    mz = {(s, same): message() for s in range(SIDE) for same in (True, False) if s or not same}

    loads[3].wait()
    valid = dm[...].astype(jnp.float32)
    key = valid * (LD - lax.broadcasted_iota(jnp.int32, (NQ, LD), 1)).astype(jnp.float32)
    key_t = jnp.transpose(jnp.concatenate([key, jnp.zeros((8 - NQ, LD), jnp.float32)], axis=0))

    def project(docs):
        for d in docs:
            loads[5 + d].wait()
        for d in docs:
            project_one(d)

    def project_one(d):
        p = unit_rows(jnp.dot(dh[d], w[...], preferred_element_type=jnp.float32))
        col = key_t[:, d:d + 1]
        first = jnp.max(col, axis=0, keepdims=True)
        colb = jnp.broadcast_to(col, (LD, DIM))
        stand_in = jnp.sum(jnp.where(colb == first, p, 0.0), axis=0, keepdims=True)
        pbuf[d] = jnp.where(colb > 0, p, stand_in).astype(jnp.bfloat16)

    project((0, 1))
    pl.semaphore_wait(barrier, len(partners))

    for s in (1, 3, 2):
        for o in range(NQ):
            push(m1[o, s], block(o, 0), block(o, 0), moved(ORDERS[o][0], s))

    for d in (0, 1):
        push(mp[d], pbuf.at[d], pbuf.at[NQ + d], sibling)
    project((2, 3))
    for d in (2, 3):
        push(mp[d], pbuf.at[d], pbuf.at[NQ + d], sibling)

    lane = lax.broadcasted_iota(jnp.int32, (8, DIM), 1)

    def score(units):
        for u, v in zip(units[::2], units[1::2]):
            q = jnp.concatenate([row(*u)[...], row(*v)[...]], axis=0)
            best = []
            for d in range(2 * NQ):
                sim = lax.dot_general(pbuf[d], q, (((1,), (1,)), ((), ())), preferred_element_type=jnp.float32)
                peak = jnp.max(sim.reshape(LD // 8, 8, 2 * DIM), axis=0)
                best.append(jnp.max(peak, axis=0, keepdims=True))
            best = jnp.concatenate(best, axis=0)
            for i, (o, r3, r2) in enumerate((u, v)):
                t = best[:, i * DIM:(i + 1) * DIM]
                for shift in (16, 8, 4, 2, 1):
                    t = t + pltpu.roll(t, DIM - shift, 1)
                place = (o % 2) * 16 + row_of(o, r3, r2)
                t = pltpu.roll(t, place, 1)
                sacc[o // 2] = jnp.where(lane % LQ == place, t, sacc[o // 2])

    def rows(*which):
        return [(o, r3, r2) for r3, r2 in which for o in range(NQ)]

    for o in range(NQ):
        for s in (1, 3, 2):
            arrived(m1[o, s], block(o, -s))
        for s in (1, 3):
            push(m2[o, s], row(o, 0, 0), row(o, 0, 0), moved(ORDERS[o][1], s))
    for o in range(NQ):
        for s in (1, 3):
            push(m3[o, s, 0], row(o, 0, 0), row(o, 0, 0), moved(ORDERS[o][2], s))
    for d in range(NQ):
        arrived(mp[d], pbuf.at[NQ + d])
    score(rows((0, 0)))
    for o in range(NQ):
        push(m2[o, 2], row(o, 0, 0), row(o, 0, 0), moved(ORDERS[o][1], 2))

    def second(o, s):
        r = -s % SIDE
        arrived(m2[o, s], row(o, 0, r))
        for t in (1, 3):
            push(m3[o, t, r], row(o, 0, r), row(o, 0, r), moved(ORDERS[o][2], t))

    def third(o, s, r, forward):
        arrived(m3[o, s, r], row(o, -s, r))
        if forward:
            push(m4[o, r], row(o, -s, r), row(o, -s, r), moved(ORDERS[o][2], s))

    def each(fn, *calls):
        for call in calls:
            for o in range(NQ):
                fn(o, *call)

    def last(o, r):
        arrived(m4[o, r], row(o, 2, r))

    each(second, (1,), (3,))
    score(rows((0, 1), (0, 3)))
    each(third, (1, 0, True), (3, 0, False))
    each(second, (2,))
    score(rows((1, 0), (3, 0), (0, 2)))
    each(third, (1, 1, True), (3, 3, True), (3, 2, True), (1, 3, False), (3, 1, False), (1, 2, False))
    score(rows((1, 1), (1, 3), (3, 1), (3, 3), (1, 2), (3, 2)))
    each(last, (0,), (1,), (3,), (2,))
    score(rows((2, 0), (2, 1), (2, 3), (2, 2)))

    loads[4].wait()
    lane1 = lane[:1]
    sub = lax.broadcasted_iota(jnp.int32, (8, DIM), 0)

    def own_lane(o):
        c1, c2, c3 = coords(o)
        return c1 * LQ + (o % 2) * 16 + c3 * SIDE + c2

    tops, sums, positives = [], [], []
    for g in range(2):
        logit = sacc[g] / temp[0]
        top = jnp.max(logit, axis=0, keepdims=True)
        tops.append(top)
        sums.append(jnp.sum(jnp.exp(logit - top), axis=0, keepdims=True))
        mine = jnp.zeros((8, DIM), jnp.float32)
        for o in (2 * g, 2 * g + 1):
            mine = jnp.where((sub == o) & (lane == own_lane(o)), logit, mine)
        positives.append(jnp.sum(mine, axis=0, keepdims=True))
    part = jnp.concatenate(tops + sums + positives + [jnp.zeros((2, DIM), jnp.float32)], axis=0)

    def merge(parts):
        top = functools.reduce(jnp.maximum, [p[0:2] for p in parts])
        total = sum(p[2:4] * jnp.exp(p[0:2] - top) for p in parts)
        positive = sum(p[4:6] for p in parts)
        return top, total, positive

    at = here['y'] * SIDE + here['x']
    xybuf[at] = part
    gathered = list(sent)
    sent.clear()
    plane = [(sx, sy) for sy in (2, 1, 3, 0) for sx in (2, 1, 3, 0) if sx or sy]
    for sx, sy in plane:
        push(mxy[sx, sy], xybuf.at[at], xybuf.at[at], moved('x', sx, True, 'y', sy))
    for copy in gathered:
        copy.wait_send()
    for sx, sy in plane[::-1]:
        arrived(mxy[sx, sy], xybuf.at[((here['y'] - sy) % SIDE) * SIDE + (here['x'] - sx) % SIDE])
    part = jnp.concatenate([*merge([xybuf[i] for i in range(SIDE * SIDE)]), jnp.zeros((2, DIM), jnp.float32)], axis=0)
    at = here['z']
    zbuf[core * SIDE + at] = part
    for s in (2, 1, 3, 0):
        for same in (True, False):
            if s or not same:
                push(mz[s, same], zbuf.at[core * SIDE + at], zbuf.at[core * SIDE + at], moved('z', s, same))
    for s in (0, 1, 3, 2):
        for same in (True, False):
            if s or not same:
                other = core if same else 1 - core
                arrived(mz[s, same], zbuf.at[other * SIDE + (at - s) % SIDE])
    total_loss = jnp.zeros((1, 1), jnp.float32)
    for c in range(2):
        top, total, positive = merge([zbuf[c * SIDE + i] for i in range(SIDE)])
        loss = top + jnp.log(total) - positive
        total_loss = total_loss + jnp.sum(jnp.sum(loss, axis=0, keepdims=True), axis=1, keepdims=True)
        if c == 0:
            losses = loss
        else:
            losses = jnp.where(core == 0, losses, loss)
    row_loss = jnp.zeros((1, DIM), jnp.float32)
    for o in range(NQ):
        g = o // 2
        value = jnp.sum(jnp.where(lane1 == own_lane(o), losses[g:g + 1], 0.0), axis=1, keepdims=True)
        row_loss = jnp.where(lane1 == o, value, row_loss)
    out_ref[...] = jnp.concatenate([row_loss, jnp.broadcast_to(total_loss / TOTAL, (7, DIM))], axis=0)

    for copy in sent:
        copy.wait_send()


def split_result(out_ref, loss_ref, mean_ref):
    loss_ref[...] = out_ref[0, :NQ]
    mean_ref[...] = out_ref[1, :1]


def solution(mesh):
    row_spec = P(('replica', 'data2', 'data'))
    tok_spec = P(('replica', 'data2', 'data'), None, None)
    mask_spec = P(('replica', 'data2', 'data'), None)
    n_msg = 12 + 12 + 32 + 16 + 4 + 15 + 7

    def local_step(query_hidden, doc_hidden, w_proj, query_mask, doc_mask, temperature):
        out = pl.pallas_call(
            kernel,
            out_shape=jax.ShapeDtypeStruct((8, DIM), jnp.float32),
            in_specs=[pl.BlockSpec(memory_space=pltpu.HBM)] * 6,
            out_specs=pl.BlockSpec(memory_space=pltpu.VMEM),
            scratch_shapes=[
                pltpu.VMEM((NQ * LQ, HID), jnp.bfloat16),
                pltpu.VMEM((NQ, LD, HID), jnp.bfloat16),
                pltpu.VMEM((HID, DIM), jnp.bfloat16),
                pltpu.VMEM((NQ, LQ), jnp.int32),
                pltpu.VMEM((NQ, LD), jnp.int32),
                pltpu.SMEM((1,), jnp.float32),
                pltpu.VMEM((NQ, SIDE * SIDE, SIDE * LQ, DIM), jnp.bfloat16),
                pltpu.VMEM((2 * NQ, LD, DIM), jnp.bfloat16),
                pltpu.VMEM((2, 8, DIM), jnp.float32),
                pltpu.VMEM((SIDE * SIDE, 8, DIM), jnp.float32),
                pltpu.VMEM((2 * SIDE, 8, DIM), jnp.float32),
                pltpu.SemaphoreType.DMA((9,)),
                pltpu.SemaphoreType.DMA((n_msg,)),
                pltpu.SemaphoreType.DMA((n_msg,)),
            ],
            compiler_params=pltpu.CompilerParams(collective_id=0, has_side_effects=True, vmem_limit_bytes=67043328),
            name='late_interaction_loss',
        )(query_hidden.reshape(NQ * LQ, HID), doc_hidden, w_proj, query_mask, doc_mask, temperature.reshape(1))
        losses, mean = pl.pallas_call(
            split_result,
            out_shape=(jax.ShapeDtypeStruct((NQ,), jnp.float32), jax.ShapeDtypeStruct((1,), jnp.float32)),
            in_specs=[pl.BlockSpec(memory_space=pltpu.VMEM)],
            out_specs=(pl.BlockSpec(memory_space=pltpu.VMEM), pl.BlockSpec(memory_space=pltpu.VMEM)),
            name='split_result',
        )(out)
        return losses, mean

    return jax.shard_map(local_step, mesh=mesh, in_specs=(tok_spec, tok_spec, P(None, None), mask_spec, mask_spec, P()),
                         out_specs=(row_spec, P('replica')), check_vma=False)
```

```python
import functools

import jax
import jax.numpy as jnp
from jax import lax
from jax.experimental import pallas as pl
from jax.experimental.pallas import tpu as pltpu
from jax.sharding import PartitionSpec as P

MESH = pl.DeviceIdType.MESH
NQ, LQ, LD, HID, DIM = 4, 32, 512, 768, 128
SIDE = 4
TOTAL = 512
ORDERS = (('x', 'y', 'z'), ('y', 'z', 'x'), ('z', 'x', 'y'), ('z', 'y', 'x'))


def unit_rows(projected):
    square = jnp.sum(projected * projected, axis=-1, keepdims=True)
    return projected * jnp.minimum(lax.rsqrt(square), 1e12)


def kernel(qh_hbm, dh_hbm, w_hbm, qm_hbm, dm_hbm, temp_hbm, out_ref,
           qh, dh, w, qm, dm, temp, qbuf, pbuf, sacc, xybuf, zbuf,
           in_sem, send_sem, recv_sem):
    outer, inner = lax.axis_index('data2'), lax.axis_index('data')
    here = {'z': outer // SIDE, 'y': outer % SIDE, 'x': inner // 2}
    core = inner % 2

    def moved(axis, step, same_core=True, axis2='x', step2=0):
        at = dict(here)
        at[axis] = (at[axis] + step) % SIDE
        at[axis2] = (at[axis2] + step2) % SIDE
        c = core if same_core else 1 - core
        return {'data2': at['z'] * SIDE + at['y'], 'data': at['x'] * 2 + c}

    sibling = moved('x', 0, False)
    used = [0]
    sent = []

    def message():
        used[0] += 1
        return used[0] - 1

    def push(slot, src, dst, device):
        copy = pltpu.make_async_remote_copy(src_ref=src, dst_ref=dst, send_sem=send_sem.at[slot],
                                            recv_sem=recv_sem.at[slot], device_id=device, device_id_type=MESH)
        copy.start()
        sent.append(copy)

    def arrived(slot, dst):
        pltpu.make_async_remote_copy(src_ref=dst, dst_ref=dst, send_sem=send_sem.at[slot],
                                     recv_sem=recv_sem.at[slot], device_id=sibling, device_id_type=MESH).wait_recv()

    loads = [pltpu.make_async_copy(s, d, in_sem.at[i]) for i, (s, d) in enumerate(
        [(w_hbm, w), (qh_hbm, qh), (qm_hbm, qm), (dm_hbm, dm), (temp_hbm, temp)]
        + [(dh_hbm.at[d], dh.at[d]) for d in range(NQ)])]
    for load in loads:
        load.start()

    partners = [moved(a, s) for a in ('x', 'y', 'z') for s in (1, 2, 3)] + [moved('z', s, False) for s in range(SIDE)]
    barrier = pltpu.get_barrier_semaphore()
    for device in partners:
        pl.semaphore_signal(barrier, inc=1, device_id=device, device_id_type=MESH)

    def coords(o):
        return [here[a] for a in ORDERS[o]]

    def row_of(o, r3, r2):
        c1, c2, c3 = coords(o)
        return ((c3 + r3) % SIDE) * SIDE + (c2 + r2) % SIDE

    def row(o, r3, r2):
        return qbuf.at[o, row_of(o, r3, r2)]

    def block(o, r1):
        c1 = coords(o)[0]
        start = pl.multiple_of(((c1 + r1) % SIDE) * LQ, LQ)
        return qbuf.at[o, row_of(o, 0, 0), pl.ds(start, LQ)]

    loads[0].wait()
    loads[1].wait()
    loads[2].wait()
    mask_t = jnp.transpose(jnp.concatenate(
        [jnp.concatenate([qm[...].astype(jnp.float32), jnp.zeros((NQ, DIM - LQ), jnp.float32)], axis=1),
         jnp.zeros((8 - NQ, DIM), jnp.float32)], axis=0))
    q = unit_rows(jnp.dot(qh[...], w[...], preferred_element_type=jnp.float32))
    for o in range(NQ):
        keep = mask_t[:LQ, o:o + 1] > 0
        block(o, 0)[...] = jnp.where(keep, q[o * LQ:(o + 1) * LQ], 0.0).astype(jnp.bfloat16)
    sacc[...] = jnp.zeros_like(sacc)

    m1 = {(o, s): message() for o in range(NQ) for s in (1, 2, 3)}
    m2 = {(o, s): message() for o in range(NQ) for s in (1, 2, 3)}
    m3 = {(o, s, r): message() for o in range(NQ) for s in (1, 3) for r in range(SIDE)}
    m4 = {(o, r): message() for o in range(NQ) for r in range(SIDE)}
    mp = [message() for _ in range(NQ)]
    mxy = {(sx, sy): message() for sx in range(SIDE) for sy in range(SIDE) if sx or sy}
    mz = {(s, same): message() for s in range(SIDE) for same in (True, False) if s or not same}

    loads[3].wait()
    valid = dm[...].astype(jnp.float32)
    key = valid * (LD - lax.broadcasted_iota(jnp.int32, (NQ, LD), 1)).astype(jnp.float32)
    key_t = jnp.transpose(jnp.concatenate([key, jnp.zeros((8 - NQ, LD), jnp.float32)], axis=0))

    def project(docs):
        for d in docs:
            loads[5 + d].wait()
        for d in docs:
            project_one(d)

    def project_one(d):
        p = unit_rows(jnp.dot(dh[d], w[...], preferred_element_type=jnp.float32))
        col = key_t[:, d:d + 1]
        first = jnp.max(col, axis=0, keepdims=True)
        colb = jnp.broadcast_to(col, (LD, DIM))
        stand_in = jnp.sum(jnp.where(colb == first, p, 0.0), axis=0, keepdims=True)
        pbuf[d] = jnp.where(colb > 0, p, stand_in).astype(jnp.bfloat16)

    project((0, 1))
    pl.semaphore_wait(barrier, len(partners))

    for s in (1, 3, 2):
        for o in range(NQ):
            push(m1[o, s], block(o, 0), block(o, 0), moved(ORDERS[o][0], s))

    for d in (0, 1):
        push(mp[d], pbuf.at[d], pbuf.at[NQ + d], sibling)
    project((2, 3))
    for d in (2, 3):
        push(mp[d], pbuf.at[d], pbuf.at[NQ + d], sibling)

    lane = lax.broadcasted_iota(jnp.int32, (8, DIM), 1)

    def score(units):
        for u, v in zip(units[::2], units[1::2]):
            q = jnp.concatenate([row(*u)[...], row(*v)[...]], axis=0)
            best = []
            for d in range(2 * NQ):
                sim = lax.dot_general(pbuf[d], q, (((1,), (1,)), ((), ())), preferred_element_type=jnp.float32)
                peak = jnp.max(sim.reshape(LD // 8, 8, 2 * DIM), axis=0)
                best.append(jnp.max(peak, axis=0, keepdims=True))
            best = jnp.concatenate(best, axis=0)
            for i, (o, r3, r2) in enumerate((u, v)):
                t = best[:, i * DIM:(i + 1) * DIM]
                for shift in (16, 8, 4, 2, 1):
                    t = t + pltpu.roll(t, DIM - shift, 1)
                place = (o % 2) * 16 + row_of(o, r3, r2)
                t = pltpu.roll(t, place, 1)
                sacc[o // 2] = jnp.where(lane % LQ == place, t, sacc[o // 2])

    def rows(*which):
        return [(o, r3, r2) for r3, r2 in which for o in range(NQ)]

    for o in range(NQ):
        for s in (1, 3, 2):
            arrived(m1[o, s], block(o, -s))
        for s in (1, 3):
            push(m2[o, s], row(o, 0, 0), row(o, 0, 0), moved(ORDERS[o][1], s))
    for o in range(NQ):
        for s in (1, 3):
            push(m3[o, s, 0], row(o, 0, 0), row(o, 0, 0), moved(ORDERS[o][2], s))
    for d in range(NQ):
        arrived(mp[d], pbuf.at[NQ + d])
    for o in range(NQ):
        push(m2[o, 2], row(o, 0, 0), row(o, 0, 0), moved(ORDERS[o][1], 2))

    score(rows((0, 0)))
    def second(o, s):
        r = -s % SIDE
        arrived(m2[o, s], row(o, 0, r))
        for t in (1, 3):
            push(m3[o, t, r], row(o, 0, r), row(o, 0, r), moved(ORDERS[o][2], t))

    def third(o, s, r, forward):
        arrived(m3[o, s, r], row(o, -s, r))
        if forward:
            push(m4[o, r], row(o, -s, r), row(o, -s, r), moved(ORDERS[o][2], s))

    def each(fn, *calls):
        for call in calls:
            for o in range(NQ):
                fn(o, *call)

    def last(o, r):
        arrived(m4[o, r], row(o, 2, r))

    each(second, (1,), (3,))
    score(rows((0, 1), (0, 3)))
    each(second, (2,))
    each(third, (1, 0, True), (3, 0, False))
    score(rows((1, 0), (3, 0), (0, 2)))
    each(third, (1, 1, True), (3, 3, True), (3, 2, True), (1, 3, False), (3, 1, False), (1, 2, False))
    score(rows((1, 1), (1, 3), (3, 1), (3, 3), (1, 2), (3, 2)))
    each(last, (0,), (1,), (3,), (2,))
    score(rows((2, 0), (2, 1), (2, 3), (2, 2)))

    loads[4].wait()
    lane1 = lane[:1]
    sub = lax.broadcasted_iota(jnp.int32, (8, DIM), 0)

    def own_lane(o):
        c1, c2, c3 = coords(o)
        return c1 * LQ + (o % 2) * 16 + c3 * SIDE + c2

    tops, sums, positives = [], [], []
    for g in range(2):
        logit = sacc[g] / temp[0]
        top = jnp.max(logit, axis=0, keepdims=True)
        tops.append(top)
        sums.append(jnp.sum(jnp.exp(logit - top), axis=0, keepdims=True))
        mine = jnp.zeros((8, DIM), jnp.float32)
        for o in (2 * g, 2 * g + 1):
            mine = jnp.where((sub == o) & (lane == own_lane(o)), logit, mine)
        positives.append(jnp.sum(mine, axis=0, keepdims=True))
    part = jnp.concatenate(tops + sums + positives + [jnp.zeros((2, DIM), jnp.float32)], axis=0)

    def merge(parts):
        top = functools.reduce(jnp.maximum, [p[0:2] for p in parts])
        total = sum(p[2:4] * jnp.exp(p[0:2] - top) for p in parts)
        positive = sum(p[4:6] for p in parts)
        return top, total, positive

    at = here['y'] * SIDE + here['x']
    xybuf[at] = part
    gathered = list(sent)
    sent.clear()
    plane = [(sx, sy) for sy in (2, 1, 3, 0) for sx in (2, 1, 3, 0) if sx or sy]
    for sx, sy in plane:
        push(mxy[sx, sy], xybuf.at[at], xybuf.at[at], moved('x', sx, True, 'y', sy))
    for copy in gathered:
        copy.wait_send()
    for sx, sy in plane[::-1]:
        arrived(mxy[sx, sy], xybuf.at[((here['y'] - sy) % SIDE) * SIDE + (here['x'] - sx) % SIDE])
    part = jnp.concatenate([*merge([xybuf[i] for i in range(SIDE * SIDE)]), jnp.zeros((2, DIM), jnp.float32)], axis=0)
    at = here['z']
    zbuf[core * SIDE + at] = part
    for s in (2, 1, 3, 0):
        for same in (True, False):
            if s or not same:
                push(mz[s, same], zbuf.at[core * SIDE + at], zbuf.at[core * SIDE + at], moved('z', s, same))
    for s in (0, 1, 3, 2):
        for same in (True, False):
            if s or not same:
                other = core if same else 1 - core
                arrived(mz[s, same], zbuf.at[other * SIDE + (at - s) % SIDE])
    total_loss = jnp.zeros((1, 1), jnp.float32)
    for c in range(2):
        top, total, positive = merge([zbuf[c * SIDE + i] for i in range(SIDE)])
        loss = top + jnp.log(total) - positive
        total_loss = total_loss + jnp.sum(jnp.sum(loss, axis=0, keepdims=True), axis=1, keepdims=True)
        if c == 0:
            losses = loss
        else:
            losses = jnp.where(core == 0, losses, loss)
    row_loss = jnp.zeros((1, DIM), jnp.float32)
    for o in range(NQ):
        g = o // 2
        value = jnp.sum(jnp.where(lane1 == own_lane(o), losses[g:g + 1], 0.0), axis=1, keepdims=True)
        row_loss = jnp.where(lane1 == o, value, row_loss)
    out_ref[...] = jnp.concatenate([row_loss, jnp.broadcast_to(total_loss / TOTAL, (7, DIM))], axis=0)

    for copy in sent:
        copy.wait_send()


def split_result(out_ref, loss_ref, mean_ref):
    loss_ref[...] = out_ref[0, :NQ]
    mean_ref[...] = out_ref[1, :1]


def solution(mesh):
    row_spec = P(('replica', 'data2', 'data'))
    tok_spec = P(('replica', 'data2', 'data'), None, None)
    mask_spec = P(('replica', 'data2', 'data'), None)
    n_msg = 12 + 12 + 32 + 16 + 4 + 15 + 7

    def local_step(query_hidden, doc_hidden, w_proj, query_mask, doc_mask, temperature):
        out = pl.pallas_call(
            kernel,
            out_shape=jax.ShapeDtypeStruct((8, DIM), jnp.float32),
            in_specs=[pl.BlockSpec(memory_space=pltpu.HBM)] * 6,
            out_specs=pl.BlockSpec(memory_space=pltpu.VMEM),
            scratch_shapes=[
                pltpu.VMEM((NQ * LQ, HID), jnp.bfloat16),
                pltpu.VMEM((NQ, LD, HID), jnp.bfloat16),
                pltpu.VMEM((HID, DIM), jnp.bfloat16),
                pltpu.VMEM((NQ, LQ), jnp.int32),
                pltpu.VMEM((NQ, LD), jnp.int32),
                pltpu.SMEM((1,), jnp.float32),
                pltpu.VMEM((NQ, SIDE * SIDE, SIDE * LQ, DIM), jnp.bfloat16),
                pltpu.VMEM((2 * NQ, LD, DIM), jnp.bfloat16),
                pltpu.VMEM((2, 8, DIM), jnp.float32),
                pltpu.VMEM((SIDE * SIDE, 8, DIM), jnp.float32),
                pltpu.VMEM((2 * SIDE, 8, DIM), jnp.float32),
                pltpu.SemaphoreType.DMA((9,)),
                pltpu.SemaphoreType.DMA((n_msg,)),
                pltpu.SemaphoreType.DMA((n_msg,)),
            ],
            compiler_params=pltpu.CompilerParams(collective_id=0, has_side_effects=True, vmem_limit_bytes=67043328),
            name='late_interaction_loss',
        )(query_hidden.reshape(NQ * LQ, HID), doc_hidden, w_proj, query_mask, doc_mask, temperature.reshape(1))
        losses, mean = pl.pallas_call(
            split_result,
            out_shape=(jax.ShapeDtypeStruct((NQ,), jnp.float32), jax.ShapeDtypeStruct((1,), jnp.float32)),
            in_specs=[pl.BlockSpec(memory_space=pltpu.VMEM)],
            out_specs=(pl.BlockSpec(memory_space=pltpu.VMEM), pl.BlockSpec(memory_space=pltpu.VMEM)),
            name='split_result',
        )(out)
        return losses, mean

    return jax.shard_map(local_step, mesh=mesh, in_specs=(tok_spec, tok_spec, P(None, None), mask_spec, mask_spec, P()),
                         out_specs=(row_spec, P('replica')), check_vma=False)
```
